32 devices in a mesh: seq: 8 (over z, y), grp: 4 (over x, core).
Axes of the slice: x: 2, y: 2, z: 4, core: 2. Of those that a mesh axis runs over, the one named last changes fastest.
Arguments:
- queries: bfloat16 [4096, 1024], P(('grp', 'seq')), may hold values from -160 to 160
- states: bfloat16 [4096, 1024], P(('grp', 'seq')), may hold values from -6 to 6
- behavior_keys: bfloat16 [8, 2048, 1024], P('grp', 'seq'), may hold values from -7 to 7
- behavior_values: bfloat16 [8, 2048, 1024], P('grp', 'seq'), may hold values from -6 to 6
- lengths: int32 [8], P('grp'), may hold values from 512 to 2048, as said below
- user_of: int32 [4096], P('grp'), may hold values from 0 to 1
- out_weight: bfloat16 [1024, 1024], replicated, may hold values from -0.1875 to 0.1875
- norm_gain: float32 [1024], replicated, may hold values from 0.1 to 1.9
- routes: int32 [4096, 2], P(('grp', 'seq')), may hold values from 0 to 31, all different within a row; in each aligned block of 256 rows (0 to 255, 256 to 511, ...) at most 16 rows name the same one
- route_weights: float32 [4096, 2], P(('grp', 'seq')), may hold values from 0.25 to 1
- expert_up: bfloat16 [32, 1024, 4096], P(('seq', 'grp')), may hold values from -0.1875 to 0.1875
- expert_down: bfloat16 [32, 4096, 1024], P(('seq', 'grp')), may hold values from -0.09375 to 0.09375
Outputs:
- block_out: bfloat16 [4096, 1024], P(('grp', 'seq'))
The draws below stay inside these ranges and needn't reach their ends.
Inputs may be any that keep to these rules, and one draw needn't show every extreme that they name: For the tokens of one device, no expert is named by more than 16 of their routes. `lengths`: some user has all 2048 behaviors valid in every draw.
All inputs are finite; a program needn't handle non-finite values.
Results may differ from the reference program's by a relative error of at most 0.0065.
Values may be sent and summed in bfloat16 or wider, within the bound.
A program may use at most 128 MiB of HBM per device.

```python
import math
import jax
import jax.numpy as jnp
import numpy as np
from jax import lax

D = 1024
HEADS = 8
HEAD_DIM = 128
FF = 4096
TOP = 2
USR_GRP = 2
TOK_DEV = 128
CAP = 16
USERS = 8
HIST = 2048
TOKENS = 4096
EXPERTS = 32


def user_table(key):
    return jax.random.randint(jax.random.fold_in(key, 71), (TOKENS,), 0, USR_GRP).astype(jnp.int32)


def key_table(key):
    return jax.random.truncated_normal(jax.random.fold_in(key, 72), -6.0, 6.0, (USERS, HIST, D), jnp.float32)


def draw_behavior_keys(key, part):
    table = key_table(key)
    return table.astype(jnp.bfloat16)


def draw_queries(key, part):
    rows = jax.random.truncated_normal(jax.random.fold_in(key, 76), -6.0, 6.0, (TOKENS, D), jnp.float32)
    return rows.astype(jnp.bfloat16)


def draw_user_of(key, part):
    return user_table(key)


def draw_lengths(key, part):
    drawn = jax.random.randint(jax.random.fold_in(key, 77), (USERS,), HIST // 4, HIST + 1).astype(jnp.int32)
    fullest = jax.random.randint(jax.random.fold_in(key, 78), (), 0, USERS).astype(jnp.int32)
    return drawn.at[fullest].set(HIST)


def block_levels(own_key, extent, cuts, smallest, top_value):
    factor_of = 1.0
    for position, shards_of in cuts:
        steps = jax.random.uniform(jax.random.fold_in(jax.random.fold_in(own_key, 6), position), (shards_of,), jnp.float32, smallest / len(cuts), top_value / len(cuts))
        factor_of = factor_of * jnp.repeat(jnp.exp(steps), extent[position] // shards_of).reshape((-1,) + (1,) * (len(extent) - 1 - position))
    return factor_of


def routed_block(key, own, number, rows, amount, top, bound, skew):
    order = jax.random.permutation(key, amount)
    crowded, usual = portions_of(amount, rows * top, bound, skew, True), portions_of(amount, rows * top, bound, skew, False)
    places = jnp.arange(amount)

    def named(sizes, offset_by):
        used = int((sizes > 0).sum())
        fixed = max(1, used // 4)
        passed = fixed + (places - fixed + offset_by * (used - fixed)) % max(1, amount - fixed)
        return jnp.zeros((amount,), jnp.int32).at[order[jnp.where(places < fixed, places, passed)]].set(jnp.asarray(sizes, jnp.int32))

    sizes = jnp.where(number % 4 == 0, named(crowded, number // 4), named(usual, number - number // 4 - 1))
    mixed = jax.random.permutation(jax.random.fold_in(own, 3), amount)
    source_of, sink = mixed[0:amount // 2 * 2:2], mixed[1:amount // 2 * 2:2]
    margin = jnp.minimum(sizes[source_of] - 1, bound - sizes[sink]) // 2
    margin = jnp.where((source_of == order[0]) | (sink == order[0]) | (sizes[sink] == 0), 0, jnp.maximum(margin, 0))
    passed = jax.random.randint(jax.random.fold_in(own, 4), (amount // 2,), 0, 1 << 20) % (margin + 1)
    sizes = sizes.at[source_of].add(-passed).at[sink].add(passed)
    items = jnp.searchsorted(jnp.cumsum(sizes), jnp.arange(rows * top), side="right").astype(jnp.int32)
    table = items.reshape(top, rows).T
    table = table[jax.random.permutation(jax.random.fold_in(own, 1), rows)]
    offset_by = jax.random.randint(jax.random.fold_in(own, 2), (rows, 1), 0, top)
    return jnp.take_along_axis(table, (jnp.arange(top)[None, :] + offset_by) % top, axis=1)


def portions_of(number_of, total, most, lean, full):
    weights = [(1 << 20) // math.isqrt(rank ** lean) + 1 for rank in range(1, number_of + 1)]
    largest = most if full else min(most, max(-(-total // number_of), total * weights[0] // sum(weights)))
    least = 1 if total - largest >= number_of - 1 else 0
    holding, rest = [largest] + [least] * (number_of - 1), total - largest - least * (number_of - 1)
    while rest > 0:
        movable = [i for i in range(1, number_of) if holding[i] < largest] or [i for i in range(1, number_of) if holding[i] < most]
        whole, budget = sum([weights[i] for i in movable]), rest
        for i in movable:
            more = min(most - holding[i], max(1, budget * weights[i] // whole), rest)
            holding[i] = holding[i] + more
            rest = rest - more
    return np.array(holding)


def centred(key, shape, scale, most, shards=(), held_as=jnp.bfloat16):
    factor_of = block_levels(key, shape, shards, -0.22, 0.18) if shards else 1.0
    values = jax.random.normal(key, shape, jnp.float32) * scale * factor_of
    return jnp.minimum(jnp.maximum(values, -most), most).astype(held_as)


def setup_inputs(seed: int = 0) -> dict:
    key_list = jax.random.split(jax.random.key(seed), 13)
    queries = draw_queries(jax.random.fold_in(key_list[12], 71), 0)
    states = centred(key_list[1], (TOKENS, D), 1.0, 6.0, ((0, 32),))
    behavior_keys = draw_behavior_keys(jax.random.fold_in(key_list[12], 71), 0)
    behavior_values = centred(key_list[3], (USERS, HIST, D), 1.0, 6.0, ((0, 4), (1, 8)))
    lengths = draw_lengths(jax.random.fold_in(key_list[12], 71), 0)
    user_of = draw_user_of(jax.random.fold_in(key_list[12], 71), 0)
    out_weight = centred(key_list[6], (D, D), D ** -0.5, 0.1875)
    norm_gain = jnp.clip(1.0 + 0.18 * jax.random.normal(key_list[7], (D,), jnp.float32), 0.1, 1.9)
    routes_keys = jax.random.split(jax.random.fold_in(key_list[8], 1), TOKENS // (TOK_DEV * TOP))
    routes_turns = jax.random.permutation(jax.random.fold_in(key_list[8], 3), TOKENS // (TOK_DEV * TOP))
    routes = jax.vmap(lambda own, number: routed_block(jax.random.fold_in(key_list[8], 2), own, number, TOK_DEV * TOP, EXPERTS, TOP, CAP, 2))(routes_keys, routes_turns).reshape((TOKENS, TOP))
    route_weights = jnp.clip(jnp.exp(math.log(1.0) - 1.3862944 * jax.random.uniform(key_list[9], (TOKENS, TOP), jnp.float32) ** block_levels(key_list[9], (TOKENS, TOP), ((0, 32),), -0.2, 0.2)), 0.25, 1.0)
    expert_up = centred(key_list[10], (EXPERTS, D, FF), D ** -0.5, 0.1875, ((0, 32),))
    expert_down = centred(key_list[11], (EXPERTS, FF, D), FF ** -0.5, 0.09375, ((0, 32),))
    return {"queries": queries, "states": states, "behavior_keys": behavior_keys, "behavior_values": behavior_values, "lengths": lengths, "user_of": user_of, "out_weight": out_weight, "norm_gain": norm_gain, "routes": routes, "route_weights": route_weights, "expert_up": expert_up, "expert_down": expert_down}


def attend_group(query_rows, owners, key_rows, value_rows, lengths):
    count = query_rows.shape[0]
    query_heads = query_rows.reshape(count, HEADS, HEAD_DIM).astype(jnp.float32)
    key_heads = key_rows.reshape(USR_GRP, HIST, HEADS, HEAD_DIM).astype(jnp.float32)
    value_heads = value_rows.reshape(USR_GRP, HIST, HEADS, HEAD_DIM).astype(jnp.float32)
    positions = jnp.arange(HIST, dtype=jnp.int32)
    factor = 1.0 / math.sqrt(HEAD_DIM)
    listing = []
    for member in range(USR_GRP):
        scores = jnp.einsum('ghd,phd->ghp', query_heads, key_heads[member]) * factor
        usable = (owners == member)[:, None, None] & (positions < lengths[member])[None, None, :]
        listing.append((jnp.where(usable, scores, -1e+30), usable))
    peaks = listing[0][0].max(-1)
    for scores, usable in listing[1:]:
        peaks = jnp.maximum(peaks, scores.max(-1))
    numer = jnp.zeros((count, HEADS, HEAD_DIM), jnp.float32)
    denom = jnp.zeros((count, HEADS), jnp.float32)
    for member in range(USR_GRP):
        scores, usable = listing[member]
        probs = jnp.where(usable, jnp.exp(scores - peaks[..., None]), 0.0)
        denom = denom + probs.sum(-1)
        low = probs.astype(jnp.bfloat16).astype(jnp.float32)
        numer = numer + jnp.einsum('ghp,phd->ghd', low, value_heads[member])
    return (numer / denom[..., None]).reshape(count, D).astype(jnp.bfloat16)

def expert_apply(rows, up_matrix, down_matrix):
    hidden = jax.nn.gelu(jnp.dot(rows, up_matrix, preferred_element_type=jnp.float32)).astype(jnp.bfloat16)
    return jnp.dot(hidden, down_matrix, preferred_element_type=jnp.float32).astype(jnp.bfloat16)

def reference(queries, states, behavior_keys, behavior_values, lengths, user_of, out_weight, norm_gain, routes, route_weights, expert_up, expert_down):
    groups = USERS // USR_GRP
    per_group = TOKENS // groups
    attended = lax.map(lambda packed: attend_group(*packed), (queries.reshape(groups, per_group, D), user_of.reshape(groups, per_group), behavior_keys.reshape(groups, USR_GRP, HIST, D), behavior_values.reshape(groups, USR_GRP, HIST, D), lengths.reshape(groups, USR_GRP)))
    attended = attended.reshape(TOKENS, D)
    residual = states.astype(jnp.float32) + jnp.dot(attended, out_weight, preferred_element_type=jnp.float32)
    spread = lax.optimization_barrier(jnp.mean(residual * residual, axis=-1, keepdims=True))
    normed = (residual / jnp.sqrt(spread + 1e-06) * norm_gain).astype(jnp.bfloat16)
    blocks = TOKENS // TOK_DEV
    width = TOK_DEV * TOP
    flat = routes.reshape(blocks, width)
    onehot = (flat[:, :, None] == jnp.arange(EXPERTS, dtype=jnp.int32)[None, None, :]).astype(jnp.int32)
    earlier = jnp.cumsum(onehot, axis=1) - onehot
    slots = lax.optimization_barrier(jnp.sum(earlier * onehot, axis=2))
    block_ids = jnp.arange(blocks, dtype=jnp.int32)[:, None]
    target = (flat * (blocks * CAP) + block_ids * CAP + slots).reshape(-1).astype(jnp.int32)
    rows = jnp.broadcast_to(normed[:, None, :], (TOKENS, TOP, D)).reshape(-1, D)
    buffer = jnp.zeros((EXPERTS * blocks * CAP, D), jnp.bfloat16).at[target].set(rows)
    buffer = buffer.reshape(EXPERTS, blocks * CAP, D)
    answered = lax.map(lambda packed: expert_apply(*packed), (buffer, expert_up, expert_down))
    picked = answered.reshape(-1, D)[target].astype(jnp.float32).reshape(TOKENS, TOP, D)
    mixed = lax.optimization_barrier(jnp.sum(picked * route_weights[:, :, None], axis=1))
    return (residual + mixed).astype(jnp.bfloat16)
```

```python
import math

import jax
import jax.numpy as jnp
from jax import lax
from jax.sharding import PartitionSpec as P

HEADS = 8


def head_layout(rows, ratio):
    users, hist_local, width = rows.shape
    sub = hist_local // ratio
    shaped = rows.reshape(users, ratio, sub, HEADS, width // HEADS)
    return jnp.transpose(shaped, (3, 1, 0, 2, 4)).reshape(HEADS * ratio, users, sub, width // HEADS)


def attend_heads(queries, behavior_keys, behavior_values, lengths, user_of):
    seq_count = lax.axis_size("seq")
    ratio = seq_count // HEADS
    tok_count, width = queries.shape
    head_size = width // HEADS
    hist_local = behavior_keys.shape[1]
    sub = hist_local // ratio
    head = lax.axis_index("seq") // ratio
    portion = lax.axis_index("seq") % ratio
    keys_head, values_head = (
        lax.all_to_all(
            head_layout(behavior_keys, ratio), "seq", split_axis=0, concat_axis=2, tiled=True
        ),
        lax.all_to_all(
            head_layout(behavior_values, ratio), "seq", split_axis=0, concat_axis=2, tiled=True
        ),
    )
    keys_head = keys_head[0]
    values_head = values_head[0]
    spread_heads = jnp.repeat(queries.reshape(tok_count, HEADS, head_size), ratio, axis=1)
    query_send = jnp.transpose(spread_heads, (1, 0, 2))
    query_head = lax.all_to_all(query_send, "seq", split_axis=0, concat_axis=0, tiled=True).reshape(
        -1, head_size
    )
    positions = (
        jnp.arange(seq_count, dtype=jnp.int32)[:, None] * hist_local
        + portion * sub
        + jnp.arange(sub, dtype=jnp.int32)[None, :]
    ).reshape(-1)
    factor = 1.0 / math.sqrt(head_size)
    listing = []
    for member in range(keys_head.shape[0]):
        scores = (
            jnp.einsum(
                "gd,pd->gp", query_head, keys_head[member], preferred_element_type=jnp.float32
            )
            * factor
        )
        usable = (user_of == member)[:, None] & (positions < lengths[member])[None, :]
        listing.append((jnp.where(usable, scores, -1e30), usable))
    peak = listing[0][0].max(-1, keepdims=True)
    for scores, usable in listing[1:]:
        peak = jnp.maximum(peak, scores.max(-1, keepdims=True))
    numer = None
    denom = None
    for member in range(len(listing)):
        scores, usable = listing[member]
        probs = jnp.where(usable, jnp.exp(scores - peak), 0.0)
        term = jnp.dot(
            probs.astype(jnp.bfloat16), values_head[member], preferred_element_type=jnp.float32
        )
        total = probs.sum(-1, keepdims=True)
        numer, denom = (term, total) if numer is None else (numer + term, denom + total)
    if ratio == 1:
        part = (numer / denom).astype(jnp.bfloat16)
    else:
        part = (numer / jnp.maximum(denom, 1e-30)).astype(jnp.bfloat16)
    part = lax.all_to_all(
        part.reshape(seq_count, tok_count, head_size), "seq", split_axis=0, concat_axis=0, tiled=True
    )
    if ratio == 1:
        return jnp.transpose(part, (1, 0, 2)).reshape(tok_count, width)
    level = jnp.where(denom > 0, peak + jnp.log(jnp.maximum(denom, 1e-30)), -1e30)
    level = lax.all_to_all(
        level.reshape(seq_count, tok_count, 1), "seq", split_axis=0, concat_axis=0, tiled=True
    ).reshape(HEADS, ratio, tok_count, 1)
    share = jax.nn.softmax(level, axis=1)
    part = part.reshape(HEADS, ratio, tok_count, head_size).astype(jnp.float32)
    joined = (part * share).sum(1)
    return jnp.transpose(joined, (1, 0, 2)).reshape(tok_count, width).astype(jnp.bfloat16)


def body(
    queries,
    states,
    behavior_keys,
    behavior_values,
    lengths,
    user_of,
    out_weight,
    norm_gain,
    routes,
    route_weights,
    expert_up,
    expert_down,
):
    tok_count = queries.shape[0]
    attended = attend_heads(queries, behavior_keys, behavior_values, lengths, user_of)
    residual = states.astype(jnp.float32) + jnp.dot(
        attended, out_weight, preferred_element_type=jnp.float32
    )
    spread = jnp.mean(residual * residual, axis=-1, keepdims=True)
    normed = (residual / jnp.sqrt(spread + 1e-06) * norm_gain).astype(jnp.bfloat16)
    seq_count = lax.axis_size("seq")
    grp_count = lax.axis_size("grp")
    experts_all = seq_count * grp_count
    width = normed.shape[1]
    top = routes.shape[1]
    capacity = max(2, 2 * tok_count * top // experts_all)
    flat = routes.reshape(-1)
    onehot = (flat[:, None] == jnp.arange(experts_all, dtype=jnp.int32)[None, :]).astype(jnp.int32)
    earlier = jnp.cumsum(onehot, axis=0) - onehot
    slots = jnp.sum(earlier * onehot, axis=1)
    target = flat * capacity + slots
    rows = jnp.broadcast_to(normed[:, None, :], (tok_count, top, width)).reshape(-1, width)
    buffer = jnp.zeros((experts_all * capacity, width), jnp.bfloat16).at[target].set(rows)
    sent = lax.all_to_all(
        buffer.reshape(experts_all, capacity, width),
        ("seq", "grp"),
        split_axis=0,
        concat_axis=0,
        tiled=True,
    )
    shape = sent.shape
    flat_rows = sent.reshape(-1, shape[-1])
    hidden = jax.nn.gelu(
        jnp.dot(flat_rows, expert_up[0], preferred_element_type=jnp.float32)
    ).astype(jnp.bfloat16)
    received = (
        jnp.dot(hidden, expert_down[0], preferred_element_type=jnp.float32)
        .astype(jnp.bfloat16)
        .reshape(shape)
    )
    answered = lax.all_to_all(received, ("seq", "grp"), split_axis=0, concat_axis=0, tiled=True)
    picked = answered.reshape(-1, width)[target].astype(jnp.float32).reshape(tok_count, top, width)
    mixed = jnp.sum(picked * route_weights[:, :, None], axis=1)
    return (residual + mixed).astype(jnp.bfloat16)


def solution(mesh):
    return jax.shard_map(
        body,
        mesh=mesh,
        in_specs=(
            P(("grp", "seq"), None),
            P(("grp", "seq"), None),
            P("grp", "seq", None),
            P("grp", "seq", None),
            P("grp"),
            P("grp"),
            P(),
            P(),
            P(("grp", "seq"), None),
            P(("grp", "seq"), None),
            P(("seq", "grp"), None, None),
            P(("seq", "grp"), None, None),
        ),
        out_specs=P(("grp", "seq"), None),
        check_vma=False,
    )
```

```python
import functools
import math

import jax
import jax.numpy as jnp
from jax import lax
from jax.experimental import pallas as pl
from jax.experimental.pallas import tpu as pltpu
from jax.sharding import PartitionSpec as P

HEADS = 8
MESH = pl.DeviceIdType.MESH


def head_layout(rows, ratio):
    users, hist_local, width = rows.shape
    sub = hist_local // ratio
    shaped = rows.reshape(users, ratio, sub, HEADS, width // HEADS)
    return jnp.transpose(shaped, (3, 1, 0, 2, 4)).reshape(HEADS * ratio, users, sub, width // HEADS)


def attend_heads(queries, behavior_keys, behavior_values, lengths, user_of):
    seq_count = lax.axis_size("seq")
    ratio = seq_count // HEADS
    tok_count, width = queries.shape
    head_size = width // HEADS
    hist_local = behavior_keys.shape[1]
    sub = hist_local // ratio
    head = lax.axis_index("seq") // ratio
    portion = lax.axis_index("seq") % ratio
    keys_head, values_head = (
        lax.all_to_all(
            head_layout(behavior_keys, ratio), "seq", split_axis=0, concat_axis=2, tiled=True
        ),
        lax.all_to_all(
            head_layout(behavior_values, ratio), "seq", split_axis=0, concat_axis=2, tiled=True
        ),
    )
    keys_head = keys_head[0]
    values_head = values_head[0]
    spread_heads = jnp.repeat(queries.reshape(tok_count, HEADS, head_size), ratio, axis=1)
    query_send = jnp.transpose(spread_heads, (1, 0, 2))
    query_head = lax.all_to_all(query_send, "seq", split_axis=0, concat_axis=0, tiled=True).reshape(
        -1, head_size
    )
    positions = (
        jnp.arange(seq_count, dtype=jnp.int32)[:, None] * hist_local
        + portion * sub
        + jnp.arange(sub, dtype=jnp.int32)[None, :]
    ).reshape(-1)
    factor = 1.0 / math.sqrt(head_size)
    listing = []
    for member in range(keys_head.shape[0]):
        scores = (
            jnp.einsum(
                "gd,pd->gp", query_head, keys_head[member], preferred_element_type=jnp.float32
            )
            * factor
        )
        usable = (user_of == member)[:, None] & (positions < lengths[member])[None, :]
        listing.append((jnp.where(usable, scores, -1e30), usable))
    peak = listing[0][0].max(-1, keepdims=True)
    for scores, usable in listing[1:]:
        peak = jnp.maximum(peak, scores.max(-1, keepdims=True))
    numer = None
    denom = None
    for member in range(len(listing)):
        scores, usable = listing[member]
        probs = jnp.where(usable, jnp.exp(scores - peak), 0.0)
        term = jnp.dot(
            probs.astype(jnp.bfloat16), values_head[member], preferred_element_type=jnp.float32
        )
        total = probs.sum(-1, keepdims=True)
        numer, denom = (term, total) if numer is None else (numer + term, denom + total)
    if ratio == 1:
        part = (numer / denom).astype(jnp.bfloat16)
    else:
        part = (numer / jnp.maximum(denom, 1e-30)).astype(jnp.bfloat16)
    part = lax.all_to_all(
        part.reshape(seq_count, tok_count, head_size), "seq", split_axis=0, concat_axis=0, tiled=True
    )
    if ratio == 1:
        return jnp.transpose(part, (1, 0, 2)).reshape(tok_count, width)
    level = jnp.where(denom > 0, peak + jnp.log(jnp.maximum(denom, 1e-30)), -1e30)
    level = lax.all_to_all(
        level.reshape(seq_count, tok_count, 1), "seq", split_axis=0, concat_axis=0, tiled=True
    ).reshape(HEADS, ratio, tok_count, 1)
    share = jax.nn.softmax(level, axis=1)
    part = part.reshape(HEADS, ratio, tok_count, head_size).astype(jnp.float32)
    joined = (part * share).sum(1)
    return jnp.transpose(joined, (1, 0, 2)).reshape(tok_count, width).astype(jnp.bfloat16)


def mega_kernel(
    seq_count,
    grp_count,
    cap,
    lengths_ref,
    q_ref,
    k_ref,
    v_ref,
    up_ref,
    down_ref,
    wo_ref,
    user_ref,
    states_ref,
    gain_ref,
    rcol_ref,
    rrow_ref,
    rw_ref,
    out_ref,
    qbuf,
    kbuf,
    vbuf,
    sbuf,
    pbuf,
    mbuf,
    lbuf,
    acc,
    osend,
    att,
    res,
    wo_v,
    up_v,
    down_v,
    dsend,
    drecv,
    rsend,
    ans,
    facc,
    wsem,
    lsem,
    qs,
    qr,
    ks,
    kr,
    vs,
    vr,
    os_,
    or_,
    ds_,
    dr_,
    rs_,
    rr_,
):
    n = seq_count
    experts = seq_count * grp_count
    tok = states_ref.shape[0]
    width = states_ref.shape[1]
    users, hist, hd = kbuf.shape[1:]
    total = n * tok
    me = lax.axis_index("seq")
    mine = lax.axis_index("grp")
    lin = me * grp_count + mine
    loads = [
        pltpu.make_async_copy(wo_ref, wo_v, wsem.at[0]),
        pltpu.make_async_copy(up_ref.at[0], up_v, wsem.at[1]),
        pltpu.make_async_copy(down_ref.at[0], down_v, wsem.at[2]),
    ]

    barrier = pltpu.get_barrier_semaphore()

    def greet(d, carry):
        peer = lax.rem(lin + d, experts)
        pl.semaphore_signal(
            barrier,
            inc=1,
            device_id={"seq": lax.div(peer, grp_count), "grp": lax.rem(peer, grp_count)},
            device_id_type=MESH,
        )
        return carry

    lax.fori_loop(1, experts, greet, 0)
    pl.semaphore_wait(barrier, experts - 1)

    def head_cols(index):
        return pl.ds(pl.multiple_of(index * hd, hd), hd)

    def tok_rows(index):
        return pl.ds(pl.multiple_of(index * tok, tok), tok)

    own = [
        pltpu.make_async_copy(q_ref.at[:, head_cols(me)], qbuf.at[tok_rows(me)], lsem.at[0]),
        pltpu.make_async_copy(k_ref.at[:, :, head_cols(me)], kbuf.at[0], lsem.at[1]),
        pltpu.make_async_copy(v_ref.at[:, :, head_cols(me)], vbuf.at[0], lsem.at[2]),
    ]
    q_copies, k_copies, v_copies = [None], [None], [None]
    for d in range(1, n):
        peer = lax.rem(me + d, n)
        to = dict(device_id={"seq": peer}, device_id_type=MESH)
        q_copies.append(
            pltpu.make_async_remote_copy(
                q_ref.at[:, head_cols(peer)], qbuf.at[tok_rows(me)], qs.at[d], qr.at[d], **to
            )
        )
        k_copies.append(
            pltpu.make_async_remote_copy(
                k_ref.at[:, :, head_cols(peer)], kbuf.at[d], ks.at[d], kr.at[d], **to
            )
        )
        v_copies.append(
            pltpu.make_async_remote_copy(
                v_ref.at[:, :, head_cols(peer)], vbuf.at[d], vs.at[d], vr.at[d], **to
            )
        )
    for copy in q_copies[1:] + k_copies[1:] + v_copies[1:]:
        copy.start()
    for copy in own:
        copy.start()
    for copy in loads:
        copy.start()

    pairs = rcol_ref.shape[0]
    rcol, rrow = rcol_ref[...], rrow_ref[...]
    same = rcol == rrow
    up_i = lax.broadcasted_iota(jnp.int32, (pairs, pairs), 0)
    low_i = lax.broadcasted_iota(jnp.int32, (pairs, pairs), 1)
    slot_row = jnp.sum(jnp.where(same & (up_i < low_i), 1.0, 0.0), axis=0, keepdims=True)
    slot_col = jnp.sum(jnp.where(same & (low_i < up_i), 1.0, 0.0), axis=1, keepdims=True)
    rel_row = jnp.where(rrow >= lin, rrow - lin, rrow - lin + experts)
    rel_col = jnp.where(rcol >= lin, rcol - lin, rcol - lin + experts)
    target_row = rel_row * cap + slot_row.astype(jnp.int32)
    target_col = rel_col * cap + slot_col.astype(jnp.int32)
    top = pairs // tok

    tile = 2 * tok
    tiles = total // tile
    factor = 1.0 / math.sqrt(hd)

    def rows_of(t):
        return pl.ds(pl.multiple_of(t * tile, tile), tile)

    own[0].wait()
    for copy in q_copies[1:]:
        copy.wait_recv()
    for d in range(n):
        if d == 0:
            own[1].wait()
        else:
            k_copies[d].wait_recv()
        base = lax.rem(me - d + n, n) * hist

        def score(t, carry, d=d, base=base):
            rows = rows_of(t)
            user = user_ref[rows, :]
            keys = kbuf[d].reshape(users * hist, hd)
            both = lax.dot_general(
                qbuf[rows, :], keys, (((1,), (1,)), ((), ())), preferred_element_type=jnp.float32
            )
            picked = both[:, :hist]
            limit = jnp.full(user.shape, lengths_ref[0], jnp.int32)
            for member in range(1, users):
                here = user == member
                picked = jnp.where(here, both[:, member * hist : (member + 1) * hist], picked)
                limit = jnp.where(here, lengths_ref[member], limit)
            place = base + lax.broadcasted_iota(jnp.int32, (tile, hist), 1)
            picked = jnp.where(place < limit, picked * factor, -1e30)
            sbuf[d, rows, :] = picked
            if d == 0:
                mbuf[rows, :] = picked
            else:
                mbuf[rows, :] = jnp.maximum(mbuf[rows, :], picked)
            return carry

        lax.fori_loop(0, tiles, score, 0)

    def soften(t, carry):
        rows = rows_of(t)
        user = user_ref[rows, :]
        peak = jnp.max(mbuf[rows, :], axis=1, keepdims=True)
        count = jnp.zeros((tile, hist), jnp.float32)
        for d in range(n):
            probs = jnp.exp(sbuf[d, rows, :] - peak)
            count = count + probs
            for member in range(users):
                pbuf[d, rows, member * hist : (member + 1) * hist] = jnp.where(
                    user == member, probs, 0.0
                ).astype(jnp.bfloat16)
        lbuf[rows, :] = jnp.broadcast_to(jnp.sum(count, axis=1, keepdims=True), (tile, hd))
        return carry

    lax.fori_loop(0, tiles, soften, 0)

    for d in range(n):
        if d == 0:
            own[2].wait()
        else:
            v_copies[d].wait_recv()

        def gather(t, carry, d=d):
            rows = rows_of(t)
            term = jnp.dot(
                pbuf[d, rows, :],
                vbuf[d].reshape(users * hist, hd),
                preferred_element_type=jnp.float32,
            )
            if d > 0:
                term = acc[rows, :] + term
            if d < n - 1:
                acc[rows, :] = term
            else:
                osend[rows, :] = (term / lbuf[rows, :]).astype(jnp.bfloat16)
            return carry

        lax.fori_loop(0, tiles, gather, 0)

    o_copies = [None]
    for d in range(1, n):
        peer = lax.rem(me + d, n)
        o_copies.append(
            pltpu.make_async_remote_copy(
                osend.at[tok_rows(peer)],
                att.at[:, head_cols(me)],
                os_.at[d],
                or_.at[d],
                device_id={"seq": peer},
                device_id_type=MESH,
            )
        )
        o_copies[d].start()
    own_o = pltpu.make_async_copy(osend.at[tok_rows(me)], att.at[:, head_cols(me)], lsem.at[3])
    own_o.start()
    own_o.wait()
    loads[0].wait()
    for copy in o_copies[1:]:
        copy.wait_recv()
    residual = states_ref[...].astype(jnp.float32) + jnp.dot(
        att[...], wo_v[...], preferred_element_type=jnp.float32
    )
    res[...] = residual
    spread = jnp.mean(residual * residual, axis=-1, keepdims=True)
    normed = (residual / jnp.sqrt(spread + 1e-06) * gain_ref[...]).astype(jnp.bfloat16)

    per = min(experts, max(1, 128 // cap))
    groups = experts // per
    d_copies, r_copies = [None], [None]
    for d in range(1, experts):
        there = lax.rem(lin + d, experts)
        back = lax.rem(lin - d + experts, experts)
        d_copies.append(
            pltpu.make_async_remote_copy(
                dsend.at[d],
                drecv.at[d],
                ds_.at[d],
                dr_.at[d],
                device_id={"seq": lax.div(there, grp_count), "grp": lax.rem(there, grp_count)},
                device_id_type=MESH,
            )
        )
        r_copies.append(
            pltpu.make_async_remote_copy(
                rsend.at[d],
                ans.at[d],
                rs_.at[d],
                rr_.at[d],
                device_id={"seq": lax.div(back, grp_count), "grp": lax.rem(back, grp_count)},
                device_id_type=MESH,
            )
        )
    for group in range(groups):
        place = lax.broadcasted_iota(jnp.int32, (per * cap, tok), 0) + group * per * cap
        hit = place == target_row[:, :tok]
        for k in range(1, top):
            hit = hit | (place == target_row[:, k * tok : (k + 1) * tok])
        rows = jnp.dot(
            jnp.where(hit, 1.0, 0.0).astype(jnp.bfloat16), normed, preferred_element_type=jnp.float32
        )
        rows = rows.astype(jnp.bfloat16).reshape(per, cap, width)
        dsend[group * per : (group + 1) * per] = rows
        for d in range(group * per, (group + 1) * per):
            if d > 0:
                d_copies[d].start()
    drecv[0] = dsend[0]

    loads[1].wait()
    loads[2].wait()
    ff = up_v.shape[1]
    step = min(ff, 512)
    for group in range(groups):
        for d in range(group * per, (group + 1) * per):
            if d > 0:
                d_copies[d].wait_recv()
        facc[...] = jnp.zeros_like(facc)

        def expert(j, carry, group=group):
            cols = pl.ds(pl.multiple_of(j * step, step), step)
            x = drecv[group * per : (group + 1) * per].reshape(per * cap, width)
            hidden = jax.nn.gelu(
                jnp.dot(x, up_v[:, cols], preferred_element_type=jnp.float32)
            ).astype(jnp.bfloat16)
            facc[...] += jnp.dot(hidden, down_v[cols, :], preferred_element_type=jnp.float32)
            return carry

        lax.fori_loop(0, ff // step, expert, 0)
        rsend[group * per : (group + 1) * per] = (
            facc[...].astype(jnp.bfloat16).reshape(per, cap, width)
        )
        for d in range(group * per, (group + 1) * per):
            if d > 0:
                r_copies[d].start()
    ans[0] = rsend[0]

    slots = experts * cap
    lane = lax.broadcasted_iota(jnp.int32, (tok, slots), 1)
    mix = jnp.zeros((tok, slots), jnp.float32)
    for k in range(top):
        span = slice(k * tok, (k + 1) * tok)
        mix = mix + jnp.where(lane == target_col[span, :], rw_ref[span, :], 0.0)
    high = mix.astype(jnp.bfloat16)
    rest = (mix - high.astype(jnp.float32)).astype(jnp.bfloat16)
    for copy in r_copies[1:]:
        copy.wait_recv()
    got = ans[...].reshape(slots, width)
    mixed = jnp.dot(high, got, preferred_element_type=jnp.float32) + jnp.dot(
        rest, got, preferred_element_type=jnp.float32
    )
    out_ref[...] = (res[...] + mixed).astype(jnp.bfloat16)
    for copy in q_copies[1:] + k_copies[1:] + v_copies[1:] + o_copies[1:]:
        copy.wait_send()
    for copy in d_copies[1:] + r_copies[1:]:
        copy.wait_send()


def fused(
    cap,
    queries,
    states,
    behavior_keys,
    behavior_values,
    lengths,
    user_of,
    out_weight,
    norm_gain,
    routes,
    route_weights,
    expert_up,
    expert_down,
):
    n = lax.axis_size("seq")
    grp_count = lax.axis_size("grp")
    experts = n * grp_count
    tok, width = queries.shape
    users, hist = behavior_keys.shape[:2]
    ff = expert_up.shape[2]
    hd = width // HEADS
    total = n * tok
    per = min(experts, max(1, 128 // cap))
    bf, f32 = jnp.bfloat16, jnp.float32
    vmem = pl.BlockSpec(memory_space=pltpu.VMEM)
    hbm = pl.BlockSpec(memory_space=pl.ANY)
    dma = pltpu.SemaphoreType.DMA
    rflat = routes.T.reshape(-1)
    return pl.pallas_call(
        functools.partial(mega_kernel, n, grp_count, cap),
        out_shape=jax.ShapeDtypeStruct((tok, width), bf),
        in_specs=[pl.BlockSpec(memory_space=pltpu.SMEM)] + [hbm] * 6 + [vmem] * 6,
        out_specs=vmem,
        scratch_shapes=[
            pltpu.VMEM((total, hd), bf),
            pltpu.VMEM((n, users, hist, hd), bf),
            pltpu.VMEM((n, users, hist, hd), bf),
            pltpu.VMEM((n, total, hist), f32),
            pltpu.VMEM((n, total, users * hist), bf),
            pltpu.VMEM((total, hist), f32),
            pltpu.VMEM((total, hd), f32),
            pltpu.VMEM((total, hd), f32),
            pltpu.VMEM((total, hd), bf),
            pltpu.VMEM((tok, width), bf),
            pltpu.VMEM((tok, width), f32),
            pltpu.VMEM(out_weight.shape, bf),
            pltpu.VMEM((width, ff), bf),
            pltpu.VMEM((ff, width), bf),
            pltpu.VMEM((experts, cap, width), bf),
            pltpu.VMEM((experts, cap, width), bf),
            pltpu.VMEM((experts, cap, width), bf),
            pltpu.VMEM((experts, cap, width), bf),
            pltpu.VMEM((per * cap, width), f32),
            dma((3,)),
            dma((4,)),
        ]
        + [dma((n,))] * 8
        + [dma((experts,))] * 4,
        compiler_params=pltpu.CompilerParams(
            collective_id=0, has_side_effects=True, vmem_limit_bytes=58 * 2**20
        ),
    )(
        lengths,
        queries,
        behavior_keys,
        behavior_values,
        expert_up,
        expert_down,
        out_weight,
        user_of.reshape(total, 1),
        states,
        norm_gain.reshape(1, width),
        rflat.reshape(-1, 1),
        rflat.reshape(1, -1),
        route_weights.T.reshape(-1, 1),
    )


def body(
    queries,
    states,
    behavior_keys,
    behavior_values,
    lengths,
    user_of,
    out_weight,
    norm_gain,
    routes,
    route_weights,
    expert_up,
    expert_down,
):
    tok_count = queries.shape[0]
    devices = lax.axis_size("seq") * lax.axis_size("grp")
    room = max(2, 2 * tok_count * routes.shape[1] // devices)
    if lax.axis_size("seq") == HEADS and room % 16 == 0:
        return fused(
            room,
            queries,
            states,
            behavior_keys,
            behavior_values,
            lengths,
            user_of,
            out_weight,
            norm_gain,
            routes,
            route_weights,
            expert_up,
            expert_down,
        )
    attended = attend_heads(queries, behavior_keys, behavior_values, lengths, user_of)
    residual = states.astype(jnp.float32) + jnp.dot(
        attended, out_weight, preferred_element_type=jnp.float32
    )
    spread = jnp.mean(residual * residual, axis=-1, keepdims=True)
    normed = (residual / jnp.sqrt(spread + 1e-06) * norm_gain).astype(jnp.bfloat16)
    seq_count = lax.axis_size("seq")
    grp_count = lax.axis_size("grp")
    experts_all = seq_count * grp_count
    width = normed.shape[1]
    top = routes.shape[1]
    capacity = max(2, 2 * tok_count * top // experts_all)
    flat = routes.reshape(-1)
    onehot = (flat[:, None] == jnp.arange(experts_all, dtype=jnp.int32)[None, :]).astype(jnp.int32)
    earlier = jnp.cumsum(onehot, axis=0) - onehot
    slots = jnp.sum(earlier * onehot, axis=1)
    target = flat * capacity + slots
    rows = jnp.broadcast_to(normed[:, None, :], (tok_count, top, width)).reshape(-1, width)
    buffer = jnp.zeros((experts_all * capacity, width), jnp.bfloat16).at[target].set(rows)
    sent = lax.all_to_all(
        buffer.reshape(experts_all, capacity, width),
        ("seq", "grp"),
        split_axis=0,
        concat_axis=0,
        tiled=True,
    )
    shape = sent.shape
    flat_rows = sent.reshape(-1, shape[-1])
    hidden = jax.nn.gelu(
        jnp.dot(flat_rows, expert_up[0], preferred_element_type=jnp.float32)
    ).astype(jnp.bfloat16)
    received = (
        jnp.dot(hidden, expert_down[0], preferred_element_type=jnp.float32)
        .astype(jnp.bfloat16)
        .reshape(shape)
    )
    answered = lax.all_to_all(received, ("seq", "grp"), split_axis=0, concat_axis=0, tiled=True)
    picked = answered.reshape(-1, width)[target].astype(jnp.float32).reshape(tok_count, top, width)
    mixed = jnp.sum(picked * route_weights[:, :, None], axis=1)
    return (residual + mixed).astype(jnp.bfloat16)


def solution(mesh):
    return jax.shard_map(
        body,
        mesh=mesh,
        in_specs=(
            P(("grp", "seq"), None),
            P(("grp", "seq"), None),
            P("grp", "seq", None),
            P("grp", "seq", None),
            P("grp"),
            P("grp"),
            P(),
            P(),
            P(("grp", "seq"), None),
            P(("grp", "seq"), None),
            P(("seq", "grp"), None, None),
            P(("seq", "grp"), None, None),
        ),
        out_specs=P(("grp", "seq"), None),
        check_vma=False,
    )
```
